32 devices in a mesh: row: 4 (over x, core), col: 8 (over z, y).
Axes of the slice: x: 2, y: 2, z: 4, core: 2. Of those that a mesh axis runs over, the one named last changes fastest.
Arguments:
- tokens: bfloat16 [4, 1152, 8192], P('row', None, 'col'), may hold values from -64 to 64
- norm_gain: bfloat16 [8192], replicated, may hold values from 0.25 to 1.75
- w_query: bfloat16 [8192, 8192], P('row', 'col'), may hold values from -0.0625 to 0.0625
- w_keyval: bfloat16 [8192, 2048], P('row', 'col'), may hold values from -0.0625 to 0.0625
- kv_cache: bfloat16 [4, 8192, 2048], P('row', None, 'col'), may hold values from -96 to 96
- selected: int32 [4, 1152], P('row'), may hold values from 0 to 8192, as said below
- anchor: int32 [4, 16], P('row'), may hold values from 0 to 8191
Outputs:
- attended: bfloat16 [4, 1152, 8192], P('row', None, 'col')
The draws below stay inside these ranges and needn't reach their ends.
Inputs may be any that keep to these rules, and one draw needn't show every extreme that they name: Each prompt's row lists distinct positions in increasing order, followed by entries equal to 8192 in the unused slots; at least three quarters of the 1152 slots of a prompt are used and some prompt uses all of them; selected positions fall unevenly over the spans.
All inputs are finite; a program needn't handle non-finite values.
Results may differ from the reference program's by a relative error of at most 0.006.
The reference program's roundings to bfloat16 on the way count: a program that leaves them out, or rounds other values in their place, can miss the bound.
Values may be sent and summed in bfloat16 or wider, within the bound.
A program may use at most 128 MiB of HBM per device.

```python
import math
import jax
import jax.numpy as jnp
from jax import lax

D = 8192
HQ = 64
KV = 8
HD = 128
SPAN = 512
NCHUNK = 16
S_MAX = 1152
P_SIZE = 4


def draw_tokens(key, part):
    first_key = jax.random.fold_in(key, 0)
    feature_ramp = jnp.exp(jnp.linspace(math.log(0.6), math.log(1.8), D))
    sampled = jax.random.normal(first_key, (P_SIZE, S_MAX, D), jnp.float32)
    return jnp.clip(sampled * feature_ramp, -64.0, 64.0).astype(jnp.bfloat16)


def draw_kv_cache(key, part):
    first_key = jax.random.fold_in(key, 0)
    sampled = jax.random.normal(first_key, (P_SIZE, NCHUNK * SPAN, 2 * KV * HD), jnp.float32)
    return jnp.clip(sampled, -96.0, 96.0).astype(jnp.bfloat16)


def draw_selected(key, part):
    first_key, second_key, third_key, fourth_key = jax.random.split(jax.random.fold_in(key, 7), 4)
    length = NCHUNK * SPAN
    span_weight = jax.random.randint(first_key, (P_SIZE, NCHUNK), 1, 9)
    noise = jax.random.randint(second_key, (P_SIZE, length), 0, 16384)
    scores = noise * jnp.repeat(span_weight, SPAN, axis=1) * length + jnp.arange(length, dtype=jnp.int32)[None, :]
    picked = lax.top_k(scores, S_MAX)[1].astype(jnp.int32)
    used = jax.random.randint(third_key, (P_SIZE,), 3 * S_MAX // 4, S_MAX + 1)
    full_prompt = jax.random.randint(fourth_key, (), 0, P_SIZE)
    used = jnp.where(jnp.arange(P_SIZE) == full_prompt, S_MAX, used)
    live = jnp.arange(S_MAX)[None, :] < used[:, None]
    picked = jnp.where(live, picked, length)
    return jnp.sort(picked, axis=1).astype(jnp.int32)


def with_ends(entries, own_key, low, largest):
    place = [jax.random.randint(jax.random.fold_in(own_key, axis), (), 0, length) for axis, length in enumerate(entries.shape)]
    main_axis = entries.shape.index(max(entries.shape))
    neighbour = place[:main_axis] + [(place[main_axis] + 1) % entries.shape[main_axis]] + place[main_axis + 1:]
    return entries.at[tuple(place)].set(low).at[tuple(neighbour)].set(largest)


def block_scale(rng, shape, cuts, least, largest):
    gain = 1.0
    for dim, blocks in cuts:
        steps = jax.random.uniform(jax.random.fold_in(jax.random.fold_in(rng, 6), dim), (blocks,), jnp.float32, least / len(cuts), largest / len(cuts))
        gain = gain * jnp.repeat(jnp.exp(steps), shape[dim] // blocks).reshape((-1,) + (1,) * (len(shape) - 1 - dim))
    return gain


def normal_values(key, dims, deviation, most, pieces=(), held_as=jnp.bfloat16):
    loudness = block_scale(key, dims, pieces, -0.22, 0.18) if pieces else 1.0
    values = jax.random.normal(key, dims, jnp.float32) * deviation * loudness
    return jnp.minimum(jnp.maximum(values, -most), most).astype(held_as)


def setup_inputs(seed: int = 0) -> dict:
    keys = jax.random.split(jax.random.key(seed), 8)
    tokens = draw_tokens(jax.random.fold_in(keys[7], 71), 0)
    norm_gain = jnp.clip(1.0 + 0.15 * jax.random.normal(keys[1], (D,), jnp.float32), 0.25, 1.75).astype(jnp.bfloat16)
    w_query = normal_values(keys[2], (D, HQ * HD), D ** -0.5, 0.0625, ((0, 4), (1, 8)))
    w_keyval = normal_values(keys[3], (D, 2 * KV * HD), D ** -0.5, 0.0625, ((0, 4), (1, 8)))
    kv_cache = draw_kv_cache(jax.random.fold_in(keys[7], 71), 0)
    selected = draw_selected(jax.random.fold_in(keys[7], 71), 0)
    anchor = with_ends(jax.random.randint(keys[6], (P_SIZE, NCHUNK), 0, NCHUNK * SPAN), jax.random.fold_in(keys[6], 1), 0, (NCHUNK * SPAN) - 1).astype(jnp.int32)
    return dict(tokens=tokens, norm_gain=norm_gain, w_query=w_query, w_keyval=w_keyval, kv_cache=kv_cache, selected=selected, anchor=anchor)


rope_base = 500000.0
epsilon = 1e-05
masked_score = -1e+30

def angles(positions, width):
    half_width = width // 2
    exponents = jnp.arange(half_width, dtype=jnp.float32) * (-2.0 / width)
    frequency = jnp.exp(exponents * math.log(rope_base))
    phases = positions[..., None] * frequency
    phases = jnp.concatenate([phases, phases], axis=-1)
    return (jnp.cos(phases), jnp.sin(phases))

def rotate(vectors, cosine, sine_part):
    half_width = vectors.shape[-1] // 2
    turned = jnp.concatenate([-vectors[..., half_width:], vectors[..., :half_width]], axis=-1)
    return vectors * cosine + turned * sine_part

def blend_rows(table, fresh, chosen):
    return table.at[chosen].set(fresh, mode='drop')

def reference(tokens, norm_gain, w_query, w_keyval, kv_cache, selected, anchor):
    hidden = tokens.astype(jnp.float32)
    mean_square = lax.optimization_barrier(jnp.mean(hidden * hidden, axis=-1, keepdims=True))
    normed = (hidden * lax.rsqrt(mean_square + epsilon) * norm_gain.astype(jnp.float32)).astype(jnp.bfloat16)
    flattened = normed.reshape(P_SIZE * S_MAX, D)
    queries = jnp.dot(flattened, w_query, preferred_element_type=jnp.float32).reshape(P_SIZE, S_MAX, HQ, HD)
    keyval = jnp.dot(flattened, w_keyval, preferred_element_type=jnp.float32).reshape(P_SIZE, S_MAX, KV, 2, HD)
    cosine, sine_part = angles(selected.astype(jnp.float32), HD)
    cosine = cosine[:, :, None]
    sine_part = sine_part[:, :, None]
    queries = rotate(queries, cosine, sine_part).astype(jnp.bfloat16)
    fresh_key = rotate(keyval[:, :, :, 0], cosine, sine_part).astype(jnp.bfloat16)
    fresh_value = keyval[:, :, :, 1].astype(jnp.bfloat16)
    length = NCHUNK * SPAN
    offsets = (jnp.arange(NCHUNK, dtype=jnp.int32) * SPAN)[None, :] - anchor.astype(jnp.int32)
    row_offsets = jnp.repeat(offsets, SPAN, axis=1).astype(jnp.float32)
    cache_cos, cache_sin = angles(row_offsets, HD)
    stored = kv_cache.reshape(P_SIZE, length, KV, 2, HD)
    key_rows = rotate(stored[:, :, :, 0].astype(jnp.float32), cache_cos[:, :, None], cache_sin[:, :, None]).astype(jnp.bfloat16)
    value_rows = stored[:, :, :, 1]
    key_rows = jax.vmap(blend_rows)(key_rows, fresh_key, selected)
    value_rows = jax.vmap(blend_rows)(value_rows, fresh_value, selected)
    group_size = HQ // KV
    scale = HD ** (-0.5)

    def attend_prompt(operands):
        queries_one, keys_one, values_one, chosen = operands
        visible = jnp.arange(length, dtype=jnp.int32)[None, :] <= chosen[:, None]

        def attend_head(head_index):
            query_head = lax.dynamic_index_in_dim(queries_one, head_index, 1, keepdims=False)
            key_head = lax.dynamic_index_in_dim(keys_one, head_index // group_size, 1, keepdims=False)
            value_head = lax.dynamic_index_in_dim(values_one, head_index // group_size, 1, keepdims=False)
            scores = jnp.dot(query_head, key_head.T, preferred_element_type=jnp.float32) * scale
            scores = jnp.where(visible, scores, masked_score)
            peak = lax.optimization_barrier(jnp.max(scores, axis=-1, keepdims=True))
            exponentials = jnp.exp(scores - peak)
            weights = exponentials.astype(jnp.bfloat16)
            numerator = jnp.dot(weights, value_head, preferred_element_type=jnp.float32)
            return numerator / lax.optimization_barrier(jnp.sum(exponentials, axis=-1, keepdims=True))
        per_head = lax.map(attend_head, jnp.arange(HQ, dtype=jnp.int32))
        return jnp.transpose(per_head, (1, 0, 2)).reshape(S_MAX, HQ * HD)
    attended = lax.map(attend_prompt, (queries, key_rows, value_rows, selected))
    live = (selected < length)[:, :, None]
    return jnp.where(live, attended, 0.0).astype(jnp.bfloat16)
```

```python
import functools
import math

import jax
import jax.numpy as jnp
from jax import lax
from jax.experimental import pallas as pl
from jax.experimental.pallas import tpu as pltpu
from jax.sharding import PartitionSpec as P

HD = 128
SPAN = 512
PAIR = 2

rope_base = 500000.0
epsilon = 1e-05
masked_score = -1e30
MESH = pl.DeviceIdType.MESH
VMEM = pl.BlockSpec(memory_space=pltpu.VMEM)
ANY = pl.BlockSpec(memory_space=pl.ANY)


def angles(positions, width):
    half_width = width // 2
    exponents = jnp.arange(half_width, dtype=jnp.float32) * (-2.0 / width)
    frequency = jnp.exp(exponents * math.log(rope_base))
    phases = positions[..., None] * frequency
    phases = jnp.concatenate([phases, phases], axis=-1)
    return (jnp.cos(phases), jnp.sin(phases))


def turn(vectors, cosine, signed_sine):
    return vectors * cosine + pltpu.roll(vectors, HD // 2, 1) * signed_sine


def signed(sine_part):
    return sine_part * jnp.where(jnp.arange(HD) < HD // 2, -1.0, 1.0).astype(jnp.float32)


def project_kernel(
    cfg, tokens, gain, wq, wkv, cosine, sine, q_out, kv_out,
    x, weights_q, weights_kv, acc, rx, to_right, to_left, to_pair, local, w_send, w_recv,
):
    ncol, nrow, chunks = cfg
    length = ncol // PAIR
    slots, width = tokens.shape
    rows = slots // chunks
    per_row = wq.shape[0]
    q_width = wq.shape[2]
    kv_width = wkv.shape[2]
    col = lax.axis_index("col")
    row = lax.axis_index("row")
    place = lax.div(col, PAIR)
    side = lax.rem(col, PAIR)
    other = 1 - side
    has_right = place + 1 < length
    has_left = place > 0
    right = {"col": lax.rem(col + PAIR, ncol)}
    left = {"col": lax.rem(col + ncol - PAIR, ncol)}
    pair = {"col": col + 1 - 2 * side}
    row_bits = list(reversed(range(nrow.bit_length() - 1)))

    def flipped(index, bit):
        step = 2**bit
        return index + step - 2 * step * lax.rem(lax.div(index, step), 2)

    barrier = pltpu.get_barrier_semaphore()
    neighbours = [right, left, pair] + [{"row": flipped(row, bit)} for bit in row_bits]
    for device in neighbours:
        pl.semaphore_signal(barrier, inc=1, device_id=device, device_id_type=MESH)
    pl.semaphore_wait(barrier, len(neighbours))

    def span(i):
        return pl.ds(pl.multiple_of(i * rows, rows), rows)

    def block(at, which):
        return at * PAIR + which

    def moved(device, sems, sem, at, which, i, own=False):
        here = x.at[block(at, which), span(i), :]
        return pltpu.make_async_remote_copy(
            src_ref=tokens.at[span(i), :] if own else here,
            dst_ref=here,
            send_sem=sems.at[sem, i],
            recv_sem=rx.at[block(at, which), i],
            device_id=device,
            device_id_type=MESH,
        )

    def arrived(at, which, i):
        moved(pair, to_pair, 0, at, which, i).wait_recv()

    @pl.loop(0, chunks)
    def _(i):
        @pl.when(has_right)
        def _():
            moved(right, to_right, place, place, side, i, True).start()

        @pl.when(has_left)
        def _():
            moved(left, to_left, place, place, side, i, True).start()

        moved(pair, to_pair, place, place, side, i, True).start()

    def weight_copy(bit, mask, number):
        owner = row
        for b in row_bits:
            if mask & 2**b:
                owner = flipped(owner, b)
        at = pl.ds(owner * per_row, per_row)
        pairs = [(wq, weights_q), (wkv, weights_kv)]
        return [
            pltpu.make_async_remote_copy(
                src_ref=source if mask == 0 else target.at[at],
                dst_ref=target.at[at],
                send_sem=w_send.at[number, j],
                recv_sem=w_recv.at[number, j],
                device_id={"row": flipped(row, bit)},
                device_id_type=MESH,
            )
            for j, (source, target) in enumerate(pairs)
        ]

    steps = []
    masks = [0]
    for bit in row_bits:
        steps += [(bit, mask) for mask in masks]
        masks += [mask ^ 2**bit for mask in masks]
    copies = [weight_copy(bit, mask, number) for number, (bit, mask) in enumerate(steps)]
    for (bit, mask), made in zip(steps, copies):
        if mask == 0:
            for copy in made:
                copy.start()
    mine = pl.ds(row * per_row, per_row)
    own_copies = [
        pltpu.make_async_copy(tokens, x.at[col], local.at[0]),
        pltpu.make_async_copy(wq, weights_q.at[mine], local.at[1]),
        pltpu.make_async_copy(wkv, weights_kv.at[mine], local.at[2]),
    ]
    for copy in own_copies:
        copy.start()

    def hand_on(distance, i):
        def forward(at, onward_ok, onward, sems):
            arrived(at, side, i)

            @pl.when(onward_ok)
            def _():
                moved(onward, sems, at, at, side, i).start()

            if distance == 1:
                @pl.when(lax.rem(i, 2) == 0)
                def _():
                    moved(pair, to_pair, at, at, side, i).start()
            else:
                moved(pair, to_pair, at, at, side, i).start()

        @pl.when(place >= distance)
        def _():
            forward(place - distance, has_right, right, to_right)

        @pl.when(place + distance < length)
        def _():
            forward(place + distance, has_left, left, to_left)

        if distance == 1:
            arrived(place, other, i)

            @pl.when((lax.rem(i, 2) == 1) & has_right)
            def _():
                moved(right, to_right, length - 1, place, other, i).start()

            @pl.when((lax.rem(i, 2) == 1) & has_left)
            def _():
                moved(left, to_left, 0, place, other, i).start()

    def project(i):
        for at in range(length):
            @pl.when(place != at)
            def _():
                arrived(at, other, i)

        def squares(b, total):
            part = x[b, span(i), :].astype(jnp.float32)
            part = part * part
            for k in range(0, width, HD):
                total = total + part[:, k : k + HD]
            return total

        total = lax.fori_loop(0, ncol, squares, jnp.zeros((rows, HD), jnp.float32))
        mean_square = jnp.sum(total, axis=1, keepdims=True) / (ncol * width)
        scale = lax.rsqrt(mean_square + epsilon)
        acc[...] = jnp.zeros(acc.shape, jnp.float32)

        @pl.loop(0, ncol)
        def _(b):
            part = x[b, span(i), :].astype(jnp.float32)
            normed = (part * scale * gain[pl.ds(b, 1), :]).astype(jnp.bfloat16)
            acc[:, :q_width] += jnp.dot(normed, weights_q[b], preferred_element_type=jnp.float32)
            acc[:, q_width:] += jnp.dot(normed, weights_kv[b], preferred_element_type=jnp.float32)

        cos, sin = cosine[span(i), :], sine[span(i), :]
        for h in range(0, q_width, HD):
            q_out[span(i), h : h + HD] = turn(acc[:, h : h + HD], cos, sin).astype(jnp.bfloat16)
        keys = acc[:, q_width : q_width + HD]
        turned = turn(keys, cos, sin)
        if kv_width == 2 * HD:
            kv_out[span(i), HD:] = acc[:, q_width + HD :].astype(jnp.bfloat16)
        else:
            turned = jnp.where(lax.rem(col, 2) == 0, turned, keys)
        kv_out[span(i), :HD] = turned.astype(jnp.bfloat16)

    for distance in range(1, length - 1):
        @pl.loop(0, chunks)
        def _(i):
            hand_on(distance, i)

    for number, (bit, mask) in enumerate(steps):
        if mask:
            came = [m for m, (b, k) in enumerate(steps) if k ^ 2**b == mask][0]
            for copy in copies[came]:
                copy.wait_recv()
            for copy in copies[number]:
                copy.start()
    forwarded = {mask for _, mask in steps}
    for number, (bit, mask) in enumerate(steps):
        if mask ^ 2**bit not in forwarded:
            for copy in copies[number]:
                copy.wait_recv()
    for copy in own_copies:
        copy.wait()

    @pl.loop(0, chunks + 1)
    def _(i):
        @pl.when(i < chunks)
        def _():
            hand_on(length - 1, i)

        @pl.when(i > 0)
        def _():
            project(i - 1)

    @pl.loop(0, chunks)
    def _(i):
        odd = lax.rem(i, 2) == 1
        for at in range(length):
            @pl.when(has_right & (place >= at))
            def _():
                moved(right, to_right, at, at, side, i).wait_send()

            @pl.when(has_left & (place <= at))
            def _():
                moved(left, to_left, at, at, side, i).wait_send()

            near = (place - at == 1) | (at - place == 1)

            @pl.when(jnp.logical_not(near & odd))
            def _():
                moved(pair, to_pair, at, at, side, i).wait_send()

        @pl.when(odd & has_right)
        def _():
            moved(right, to_right, length - 1, place, other, i).wait_send()

        @pl.when(odd & has_left)
        def _():
            moved(left, to_left, 0, place, other, i).wait_send()

    for made in copies:
        for copy in made:
            copy.wait_send()


def gather_and_project(tokens, norm_gain, w_query, w_keyval, cosine, signed_sine):
    ncol, nrow = lax.axis_size("col"), lax.axis_size("row")
    slots, width = tokens.shape
    depth, q_width = w_query.shape
    kv_width = w_keyval.shape[1]
    chunks = next(n for n in (6, 4, 3, 2, 1) if slots % (n * 16) == 0)
    rows = slots // chunks
    features = ncol * width
    length = ncol // PAIR
    moves = nrow - 1
    dma = pltpu.SemaphoreType.DMA
    outs = (
        jax.ShapeDtypeStruct((slots, q_width), jnp.bfloat16),
        jax.ShapeDtypeStruct((slots, kv_width), jnp.bfloat16),
    )
    return pl.pallas_call(
        functools.partial(project_kernel, (ncol, nrow, chunks)),
        out_shape=outs,
        in_specs=[ANY, VMEM, ANY, ANY, VMEM, VMEM],
        out_specs=(VMEM, VMEM),
        scratch_shapes=[
            pltpu.VMEM((ncol, slots, width), jnp.bfloat16),
            pltpu.VMEM((ncol, width, q_width), jnp.bfloat16),
            pltpu.VMEM((ncol, width, kv_width), jnp.bfloat16),
            pltpu.VMEM((rows, q_width + kv_width), jnp.float32),
            dma((ncol, chunks)),
            dma((length, chunks)),
            dma((length, chunks)),
            dma((length, chunks)),
            dma((3,)),
            dma((moves, 2)),
            dma((moves, 2)),
        ],
        compiler_params=pltpu.CompilerParams(
            collective_id=0, has_side_effects=True, vmem_limit_bytes=62 * 2**20
        ),
        cost_estimate=pl.CostEstimate(
            flops=2 * slots * features * (q_width + kv_width),
            bytes_accessed=2 * (slots * features + features * (q_width + kv_width)),
            transcendentals=0,
        ),
    )(
        tokens,
        norm_gain.astype(jnp.float32).reshape(ncol, width),
        w_query.reshape(depth // width, width, q_width),
        w_keyval.reshape(depth // width, width, kv_width),
        cosine,
        signed_sine,
    )


def attend_kernel(cfg, bounds, edges, q, fresh, cache, chosen, chosen_row, acos, asin, out, kt, vx, qs, m, acc, sbuf):
    heads, length, key_size, group, pipelined = cfg
    block = pl.program_id(0)
    rows = q.shape[0]
    total_rows = heads * rows
    factor = HD ** (-0.5) * math.log2(math.e)
    spans = length // SPAN

    @pl.when(block == 0)
    def _():
        ones = jnp.ones((128, HD), jnp.bfloat16)

        def prepare(c, carry):
            base = pl.multiple_of(c * SPAN, SPAN)
            stored = cache[pl.ds(base, SPAN), :]
            keys = stored[:, :HD].astype(jnp.float32)
            turned = keys * acos[pl.ds(c, 1), :] + pltpu.roll(keys, HD // 2, 1) * asin[pl.ds(c, 1), :]
            first = edges[c] // 128
            last = (edges[c + 1] + 127) // 128

            def blend(tile, pair):
                key_rows, value_rows = pair
                at = pl.multiple_of(tile * 128, 128)
                place = base + lax.broadcasted_iota(jnp.int32, (SPAN, 128), 0)
                hits = (place == chosen_row[:, pl.ds(at, 128)]).astype(jnp.float32).astype(jnp.bfloat16)
                fresh_tile = jnp.concatenate([fresh[pl.ds(at, 128), :], ones], axis=1)
                placed = jnp.dot(hits, fresh_tile, preferred_element_type=jnp.float32)
                hit = placed[:, 2 * HD :] > 0.5
                return (
                    jnp.where(hit, placed[:, :HD], key_rows),
                    jnp.where(hit, placed[:, HD : 2 * HD], value_rows),
                )

            key_rows, value_rows = lax.fori_loop(
                first, last, blend,
                (turned.astype(jnp.bfloat16).astype(jnp.float32), stored[:, HD:].astype(jnp.float32)),
            )
            across = key_rows.T.astype(jnp.bfloat16)
            kt[:HD, pl.ds(base, SPAN)] = across
            kt[HD:, pl.ds(base, SPAN)] = across
            vx[pl.ds(base, SPAN), :HD] = value_rows.astype(jnp.bfloat16)
            vx[pl.ds(base, SPAN), HD:] = jnp.ones((SPAN, HD), jnp.bfloat16)
            return carry

        lax.fori_loop(0, spans, prepare, 0)

    for h in range(heads):
        scaled = q[:, h * HD : (h + 1) * HD].astype(jnp.float32) * factor
        high = scaled.astype(jnp.bfloat16)
        low = (scaled - high.astype(jnp.float32)).astype(jnp.bfloat16)
        qs[h * rows : (h + 1) * rows, :HD] = high
        qs[h * rows : (h + 1) * rows, HD:] = low
    m[...] = jnp.full(m.shape, masked_score, jnp.float32)
    acc[...] = jnp.zeros(acc.shape, jnp.float32)
    limit = chosen[...]
    full, total = bounds[block, 0], bounds[block, 1]
    copies = key_size // HD

    def softmax_step(index, at, scores, masked, limits):
        start = pl.multiple_of(index * key_size, key_size)
        if masked:
            place = start + lax.broadcasted_iota(jnp.int32, scores.shape, 1)
            scores = jnp.where(place <= limits, scores, masked_score)
        old = m[at : at + group, :]
        new = jnp.maximum(old, jnp.max(scores, axis=1, keepdims=True))
        rescale = jnp.exp2(old - new)
        weights = jnp.exp2(scores - jnp.concatenate([new] * copies, axis=1)).astype(jnp.bfloat16)
        part = jnp.dot(weights, vx[pl.ds(start, key_size), :], preferred_element_type=jnp.float32)
        acc[at : at + group, :] = acc[at : at + group, :] * jnp.concatenate([rescale, rescale], axis=1) + part
        m[at : at + group, :] = new

    def score(index, at):
        start = pl.multiple_of(index * key_size, key_size)
        return jnp.dot(qs[at : at + group, :], kt[:, pl.ds(start, key_size)], preferred_element_type=jnp.float32)

    if group >= rows:
        limits = jnp.concatenate([limit] * (group // rows), axis=0)
    else:
        limits = None

    def plain(masked, index, carry):
        for at in range(0, total_rows, group):
            lim = limits if limits is not None else limit[at % rows : at % rows + group, :]
            softmax_step(index, at, score(index, at), masked, lim)
        return carry

    def piped(masked, index, carry):
        slot = lax.rem(index, 2)
        nxt = jnp.minimum(index + 1, total - 1)
        for at in range(0, total_rows, group):
            lim = limits if limits is not None else limit[at % rows : at % rows + group, :]
            sbuf[1 - slot, at : at + group, :] = score(nxt, at)
            softmax_step(index, at, sbuf[slot, at : at + group, :], masked, lim)
        return carry

    if pipelined == 1:
        for at in range(0, total_rows, group):
            sbuf[0, at : at + group, :] = score(0, at)
        body = piped
    else:
        body = plain
    lax.fori_loop(0, full, functools.partial(body, False), 0)
    lax.fori_loop(full, total, functools.partial(body, True), 0)
    for h in range(heads):
        part = acc[h * rows : (h + 1) * rows, :]
        outcome = jnp.where(limit < length, part[:, :HD] / part[:, HD:], 0.0)
        out[:, h * HD : (h + 1) * HD] = outcome.astype(out.dtype)


def attend(q, fresh, cache, chosen, anchor, rows=128, key_size=512, group=256, pipelined=0):
    slot_count, width = q.shape
    length = cache.shape[0]
    heads = width // HD
    blocks = slot_count // rows
    spans = length // SPAN
    signs = jnp.where(jnp.arange(HD) < HD // 2, -1.0, 1.0).astype(jnp.float32)
    offsets = jnp.arange(spans, dtype=jnp.int32) * SPAN - anchor
    acos, asin = angles(offsets.astype(jnp.float32), HD)
    grouped = chosen.reshape(blocks, rows)
    farthest = jnp.max(jnp.where(grouped < length, grouped, 0), axis=1)
    total = farthest // key_size + 1
    full = jnp.minimum((grouped[:, 0] + 1) // key_size, total)
    bounds = jnp.stack([full, total], axis=1).astype(jnp.int32)
    marks = jnp.arange(spans + 1, dtype=jnp.int32) * SPAN
    edges = jnp.sum(chosen[None, :] < marks[:, None], axis=1).astype(jnp.int32)
    mine = lambda i, *_: (i, 0)
    whole = lambda i, *_: (0, 0)
    elements = slot_count * heads * length
    R = heads * rows
    return pl.pallas_call(
        functools.partial(attend_kernel, (heads, length, key_size, group, pipelined)),
        grid_spec=pltpu.PrefetchScalarGridSpec(
            num_scalar_prefetch=2,
            grid=(blocks,),
            in_specs=[
                pl.BlockSpec((rows, width), mine),
                pl.BlockSpec(fresh.shape, whole),
                pl.BlockSpec(cache.shape, whole),
                pl.BlockSpec((rows, 1), mine),
                pl.BlockSpec((1, slot_count), whole),
                pl.BlockSpec((spans, HD), whole),
                pl.BlockSpec((spans, HD), whole),
            ],
            out_specs=pl.BlockSpec((rows, width), mine),
            scratch_shapes=[
                pltpu.VMEM((2 * HD, length), jnp.bfloat16),
                pltpu.VMEM((length, 2 * HD), jnp.bfloat16),
                pltpu.VMEM((R, 2 * HD), jnp.bfloat16),
                pltpu.VMEM((R, HD), jnp.float32),
                pltpu.VMEM((R, 2 * HD), jnp.float32),
                pltpu.VMEM((2, R, key_size) if pipelined == 1 else (2, 8, 128), jnp.float32),
            ],
        ),
        out_shape=jax.ShapeDtypeStruct((slot_count, width), jnp.bfloat16),
        compiler_params=pltpu.CompilerParams(vmem_limit_bytes=60 * 2**20),
    )(bounds, edges, q, fresh, cache, chosen[:, None], chosen[None, :], acos, asin * signs)


def from_partner(value):
    pairs = [(source, source ^ 1) for source in range(lax.axis_size("col"))]
    return lax.ppermute(value, "col", pairs)


def shards(tokens, norm_gain, w_query, w_keyval, kv_cache, selected, anchor):
    chosen = selected[0]
    cosine, sine_part = angles(chosen.astype(jnp.float32), HD)
    queries, fresh = gather_and_project(
        tokens[0], norm_gain, w_query, w_keyval, cosine, signed(sine_part)
    )
    stored = kv_cache[0]
    if w_keyval.shape[1] == HD:
        holds_key = lax.axis_index("col") % 2 == 0

        def both(mine):
            partner = from_partner(mine)
            return jnp.concatenate(
                [jnp.where(holds_key, mine, partner), jnp.where(holds_key, partner, mine)], axis=1
            )

        stored, fresh = both(stored), both(fresh)
    return attend(queries, fresh, stored, chosen, anchor[0])[None]


def solution(mesh):
    in_specs = (
        P("row", None, "col"),
        P(),
        P("row", "col"),
        P("row", "col"),
        P("row", None, "col"),
        P("row", None),
        P("row", None),
    )
    out_specs = P("row", None, "col")
    return jax.shard_map(shards, mesh=mesh, in_specs=in_specs, out_specs=out_specs, check_vma=False)
```

```python
import functools
import math

import jax
import jax.numpy as jnp
from jax import lax
from jax.experimental import pallas as pl
from jax.experimental.pallas import tpu as pltpu
from jax.sharding import PartitionSpec as P

HD = 128
SPAN = 512
PAIR = 2
ONES = 16

rope_base = 500000.0
epsilon = 1e-05
masked_score = -1e30
MESH = pl.DeviceIdType.MESH
VMEM = pl.BlockSpec(memory_space=pltpu.VMEM)
ANY = pl.BlockSpec(memory_space=pl.ANY)


def angles(positions, width):
    half_width = width // 2
    exponents = jnp.arange(half_width, dtype=jnp.float32) * (-2.0 / width)
    frequency = jnp.exp(exponents * math.log(rope_base))
    phases = positions[..., None] * frequency
    phases = jnp.concatenate([phases, phases], axis=-1)
    return (jnp.cos(phases), jnp.sin(phases))


def turn(vectors, cosine, signed_sine):
    return vectors * cosine + pltpu.roll(vectors, HD // 2, 1) * signed_sine


def signed(sine_part):
    return sine_part * jnp.where(jnp.arange(HD) < HD // 2, -1.0, 1.0).astype(jnp.float32)


def project_kernel(
    cfg, tokens, gain, wq, wkv, cosine, sine, q_out, kv_out,
    x, weights_q, weights_kv, acc, rx, to_right, to_left, to_pair, local, w_send, w_recv,
):
    ncol, nrow, chunks = cfg
    length = ncol // PAIR
    slots, width = tokens.shape
    rows = slots // chunks
    detour = chunks // 2
    per_row = wq.shape[0]
    q_width = wq.shape[2]
    kv_width = wkv.shape[2]
    col = lax.axis_index("col")
    row = lax.axis_index("row")
    place = lax.div(col, PAIR)
    side = lax.rem(col, PAIR)
    other = 1 - side
    has_right = place + 1 < length
    has_left = place > 0
    right = {"col": lax.rem(col + PAIR, ncol)}
    left = {"col": lax.rem(col + ncol - PAIR, ncol)}
    pair = {"col": col + 1 - 2 * side}
    row_bits = list(reversed(range(nrow.bit_length() - 1)))

    def flipped(index, bit):
        step = 2**bit
        return index + step - 2 * step * lax.rem(lax.div(index, step), 2)

    barrier = pltpu.get_barrier_semaphore()
    neighbours = [right, left, pair] + [{"row": flipped(row, bit)} for bit in row_bits]
    for device in neighbours:
        pl.semaphore_signal(barrier, inc=1, device_id=device, device_id_type=MESH)
    pl.semaphore_wait(barrier, len(neighbours))

    def span(i):
        return pl.ds(pl.multiple_of(i * rows, rows), rows)

    def block(at, which):
        return at * PAIR + which

    def moved(device, sems, sem, at, which, i, own=False):
        here = x.at[block(at, which), span(i), :]
        return pltpu.make_async_remote_copy(
            src_ref=tokens.at[span(i), :] if own else here,
            dst_ref=here,
            send_sem=sems.at[sem, i],
            recv_sem=rx.at[block(at, which), i],
            device_id=device,
            device_id_type=MESH,
        )

    def arrived(at, which, i):
        moved(pair, to_pair, 0, at, which, i).wait_recv()

    @pl.loop(0, chunks)
    def _(i):
        @pl.when(has_right)
        def _():
            moved(right, to_right, place, place, side, i, True).start()

        @pl.when(has_left)
        def _():
            moved(left, to_left, place, place, side, i, True).start()

        moved(pair, to_pair, place, place, side, i, True).start()

    def weight_copy(bit, mask, number):
        owner = row
        for b in row_bits:
            if mask & 2**b:
                owner = flipped(owner, b)
        at = pl.ds(owner * per_row, per_row)
        pairs = [(wq, weights_q), (wkv, weights_kv)]
        return [
            pltpu.make_async_remote_copy(
                src_ref=source if mask == 0 else target.at[at],
                dst_ref=target.at[at],
                send_sem=w_send.at[number, j],
                recv_sem=w_recv.at[number, j],
                device_id={"row": flipped(row, bit)},
                device_id_type=MESH,
            )
            for j, (source, target) in enumerate(pairs)
        ]

    steps = []
    masks = [0]
    for bit in row_bits:
        steps += [(bit, mask) for mask in masks]
        masks += [mask ^ 2**bit for mask in masks]
    copies = [weight_copy(bit, mask, number) for number, (bit, mask) in enumerate(steps)]
    for (bit, mask), made in zip(steps, copies):
        if mask == 0:
            for copy in made:
                copy.start()
    mine = pl.ds(row * per_row, per_row)
    own_copies = [
        pltpu.make_async_copy(tokens, x.at[col], local.at[0]),
        pltpu.make_async_copy(wq, weights_q.at[mine], local.at[1]),
        pltpu.make_async_copy(wkv, weights_kv.at[mine], local.at[2]),
    ]
    for copy in own_copies:
        copy.start()

    def hand_on(distance, i):
        def forward(at, onward_ok, onward, sems):
            arrived(at, side, i)

            @pl.when(onward_ok)
            def _():
                moved(onward, sems, at, at, side, i).start()

            if distance == 1:
                @pl.when(i < detour)
                def _():
                    moved(pair, to_pair, at, at, side, i).start()
            else:
                moved(pair, to_pair, at, at, side, i).start()

        @pl.when(place >= distance)
        def _():
            forward(place - distance, has_right, right, to_right)

        @pl.when(place + distance < length)
        def _():
            forward(place + distance, has_left, left, to_left)

        if distance == 1:
            arrived(place, other, i)

    def project(i):
        for at in range(length):
            @pl.when(place != at)
            def _():
                arrived(at, other, i)

        def squares(b, total):
            part = x[b, span(i), :].astype(jnp.float32)
            part = part * part
            for k in range(0, width, HD):
                total = total + part[:, k : k + HD]
            return total

        total = lax.fori_loop(0, ncol, squares, jnp.zeros((rows, HD), jnp.float32))
        mean_square = jnp.sum(total, axis=1, keepdims=True) / (ncol * width)
        scale = lax.rsqrt(mean_square + epsilon)
        acc[...] = jnp.zeros(acc.shape, jnp.float32)

        @pl.loop(0, ncol)
        def _(b):
            part = x[b, span(i), :].astype(jnp.float32)
            normed = (part * scale * gain[pl.ds(b, 1), :]).astype(jnp.bfloat16)
            acc[:, :q_width] += jnp.dot(normed, weights_q[b], preferred_element_type=jnp.float32)
            acc[:, q_width:] += jnp.dot(normed, weights_kv[b], preferred_element_type=jnp.float32)

        cos, sin = cosine[span(i), :], sine[span(i), :]
        for h in range(0, q_width, HD):
            q_out[span(i), h : h + HD] = turn(acc[:, h : h + HD], cos, sin).astype(jnp.bfloat16)
        keys = acc[:, q_width : q_width + HD]
        turned = turn(keys, cos, sin)
        if kv_width == 2 * HD:
            kv_out[span(i), HD:] = acc[:, q_width + HD :].astype(jnp.bfloat16)
        else:
            turned = jnp.where(lax.rem(col, 2) == 0, turned, keys)
        kv_out[span(i), :HD] = turned.astype(jnp.bfloat16)

    for distance in range(1, length - 1):
        @pl.loop(0, chunks)
        def _(i):
            hand_on(distance, i)

    @pl.loop(detour, chunks)
    def _(i):
        @pl.when(has_right)
        def _():
            moved(right, to_right, length - 1, place, other, i).start()

        @pl.when(has_left)
        def _():
            moved(left, to_left, 0, place, other, i).start()

    for number, (bit, mask) in enumerate(steps):
        if mask:
            came = [m for m, (b, k) in enumerate(steps) if k ^ 2**b == mask][0]
            for copy in copies[came]:
                copy.wait_recv()
            for copy in copies[number]:
                copy.start()
    forwarded = {mask for _, mask in steps}
    for number, (bit, mask) in enumerate(steps):
        if mask ^ 2**bit not in forwarded:
            for copy in copies[number]:
                copy.wait_recv()
    for copy in own_copies:
        copy.wait()

    ahead = min(chunks, 4)

    @pl.loop(0, chunks + ahead)
    def _(i):
        @pl.when(i < chunks)
        def _():
            hand_on(length - 1, i)

        @pl.when(i >= ahead)
        def _():
            project(i - ahead)

    @pl.loop(0, chunks)
    def _(i):
        late = i >= detour
        for at in range(length):
            @pl.when(has_right & (place >= at))
            def _():
                moved(right, to_right, at, at, side, i).wait_send()

            @pl.when(has_left & (place <= at))
            def _():
                moved(left, to_left, at, at, side, i).wait_send()

            near = (place - at == 1) | (at - place == 1)

            @pl.when(jnp.logical_not(near & late))
            def _():
                moved(pair, to_pair, at, at, side, i).wait_send()

        @pl.when(late & has_right)
        def _():
            moved(right, to_right, length - 1, place, other, i).wait_send()

        @pl.when(late & has_left)
        def _():
            moved(left, to_left, 0, place, other, i).wait_send()

    for made in copies:
        for copy in made:
            copy.wait_send()


def gather_and_project(tokens, norm_gain, w_query, w_keyval, cosine, signed_sine):
    ncol, nrow = lax.axis_size("col"), lax.axis_size("row")
    slots, width = tokens.shape
    depth, q_width = w_query.shape
    kv_width = w_keyval.shape[1]
    chunks = next(n for n in (6, 4, 3, 2, 1) if slots % (n * 16) == 0)
    rows = slots // chunks
    features = ncol * width
    length = ncol // PAIR
    moves = nrow - 1
    dma = pltpu.SemaphoreType.DMA
    outs = (
        jax.ShapeDtypeStruct((slots, q_width), jnp.bfloat16),
        jax.ShapeDtypeStruct((slots, kv_width), jnp.bfloat16),
    )
    return pl.pallas_call(
        functools.partial(project_kernel, (ncol, nrow, chunks)),
        out_shape=outs,
        in_specs=[ANY, VMEM, ANY, ANY, VMEM, VMEM],
        out_specs=(VMEM, VMEM),
        scratch_shapes=[
            pltpu.VMEM((ncol, slots, width), jnp.bfloat16),
            pltpu.VMEM((ncol, width, q_width), jnp.bfloat16),
            pltpu.VMEM((ncol, width, kv_width), jnp.bfloat16),
            pltpu.VMEM((rows, q_width + kv_width), jnp.float32),
            dma((ncol, chunks)),
            dma((length, chunks)),
            dma((length, chunks)),
            dma((length, chunks)),
            dma((3,)),
            dma((moves, 2)),
            dma((moves, 2)),
        ],
        compiler_params=pltpu.CompilerParams(
            collective_id=0, has_side_effects=True, vmem_limit_bytes=62 * 2**20
        ),
        cost_estimate=pl.CostEstimate(
            flops=2 * slots * features * (q_width + kv_width),
            bytes_accessed=2 * (slots * features + features * (q_width + kv_width)),
            transcendentals=0,
        ),
    )(
        tokens,
        norm_gain.astype(jnp.float32).reshape(ncol, width),
        w_query.reshape(depth // width, width, q_width),
        w_keyval.reshape(depth // width, width, kv_width),
        cosine,
        signed_sine,
    )


def attend_kernel(cfg, bounds, edges, q, fresh, cache, chosen, chosen_row, acos, asin, out, keys, values, qt, m, acc):
    heads, length, wide, narrow, group = cfg
    block = pl.program_id(0)
    rows = q.shape[0]
    factor = HD ** (-0.5) * math.log2(math.e)
    spans = length // SPAN

    @pl.when(block == 0)
    def _():
        ones = jnp.ones((128, HD), jnp.bfloat16)

        def prepare(c, carry):
            base = pl.multiple_of(c * SPAN, SPAN)
            stored = cache[pl.ds(base, SPAN), :]
            old = stored[:, :HD].astype(jnp.float32)
            turned = old * acos[pl.ds(c, 1), :] + pltpu.roll(old, HD // 2, 1) * asin[pl.ds(c, 1), :]
            keys[pl.ds(base, SPAN), :HD] = turned.astype(jnp.bfloat16)
            keys[pl.ds(base, SPAN), HD:] = stored[:, HD:]

            def blend(tile, carry):
                at = pl.multiple_of(tile * 128, 128)
                place = base + lax.broadcasted_iota(jnp.int32, (SPAN, 128), 0)
                hits = (place == chosen_row[:, pl.ds(at, 128)]).astype(jnp.float32).astype(jnp.bfloat16)
                fresh_tile = jnp.concatenate([fresh[pl.ds(at, 128), :], ones], axis=1)
                placed = jnp.dot(hits, fresh_tile, preferred_element_type=jnp.float32)
                hit = placed[:, 2 * HD :] > 0.5
                for k in (0, HD):
                    before = keys[pl.ds(base, SPAN), k : k + HD].astype(jnp.float32)
                    after = jnp.where(hit, placed[:, k : k + HD], before)
                    keys[pl.ds(base, SPAN), k : k + HD] = after.astype(jnp.bfloat16)
                return carry

            lax.fori_loop(edges[c] // 128, (edges[c + 1] + 127) // 128, blend, 0)
            values[:HD, pl.ds(base, SPAN)] = keys[pl.ds(base, SPAN), HD:].astype(jnp.float32).T.astype(jnp.bfloat16)
            values[HD:, pl.ds(base, SPAN)] = jnp.ones((ONES, SPAN), jnp.bfloat16)
            keys[pl.ds(base, SPAN), HD:] = keys[pl.ds(base, SPAN), :HD]
            return carry

        lax.fori_loop(0, spans, prepare, 0)

    for h in range(heads):
        scaled = (q[:, h * HD : (h + 1) * HD].astype(jnp.float32) * factor).T
        high = scaled.astype(jnp.bfloat16)
        qt[:HD, h * rows : (h + 1) * rows] = high
        qt[HD:, h * rows : (h + 1) * rows] = (scaled - high.astype(jnp.float32)).astype(jnp.bfloat16)
    m[...] = jnp.full(m.shape, masked_score, jnp.float32)
    acc[...] = jnp.zeros(acc.shape, jnp.float32)
    limit = chosen[...]
    limits = jnp.concatenate([limit] * (group // rows), axis=1) if group > rows else limit

    def advance(size, masked, index, carry):
        start = pl.multiple_of(index * size, size)
        key_block = keys[pl.ds(start, size), :]
        value_block = values[:, pl.ds(start, size)]
        for at in range(0, heads * rows, group):
            scores = jnp.dot(key_block, qt[:, at : at + group], preferred_element_type=jnp.float32)
            if masked:
                place = start + lax.broadcasted_iota(jnp.int32, scores.shape, 0)
                scores = jnp.where(place <= limits, scores, masked_score)
            old = m[:, at : at + group]
            new = jnp.maximum(old, jnp.max(scores, axis=0, keepdims=True))
            weights = jnp.exp2(scores - new).astype(jnp.bfloat16)
            part = jnp.dot(value_block, weights, preferred_element_type=jnp.float32)
            acc[:, at : at + group] = acc[:, at : at + group] * jnp.exp2(old - new) + part
            m[:, at : at + group] = new
        return carry

    full, total = bounds[block, 0], bounds[block, 1]
    lax.fori_loop(0, full, functools.partial(advance, wide, False), 0)
    lax.fori_loop(full * (wide // narrow), total, functools.partial(advance, narrow, True), 0)
    for h in range(heads):
        part = acc[:, h * rows : (h + 1) * rows]
        outcome = jnp.where(limit < length, part[:HD, :] / part[HD : HD + 1, :], 0.0)
        out[:, h * HD : (h + 1) * HD] = outcome.T.astype(out.dtype)


def attend(q, fresh, cache, chosen, anchor, rows=128, wide=2048, narrow=512, group=1024):
    slot_count, width = q.shape
    length = cache.shape[0]
    heads = width // HD
    blocks = slot_count // rows
    spans = length // SPAN
    signs = jnp.where(jnp.arange(HD) < HD // 2, -1.0, 1.0).astype(jnp.float32)
    offsets = jnp.arange(spans, dtype=jnp.int32) * SPAN - anchor
    acos, asin = angles(offsets.astype(jnp.float32), HD)
    grouped = chosen.reshape(blocks, rows)
    farthest = jnp.max(jnp.where(grouped < length, grouped, 0), axis=1)
    total = farthest // narrow + 1
    full = jnp.minimum((grouped[:, 0] + 1) // wide, (farthest + 1) // wide)
    bounds = jnp.stack([full, total], axis=1).astype(jnp.int32)
    marks = jnp.arange(spans + 1, dtype=jnp.int32) * SPAN
    edges = jnp.sum(chosen[None, :] < marks[:, None], axis=1).astype(jnp.int32)
    mine = lambda i, *_: (i, 0)
    across = lambda i, *_: (0, i)
    whole = lambda i, *_: (0, 0)
    R = heads * rows
    group = min(group, R)
    wide = wide if length % wide == 0 else narrow
    elements = slot_count * heads * length
    return pl.pallas_call(
        functools.partial(attend_kernel, (heads, length, wide, narrow, group)),
        grid_spec=pltpu.PrefetchScalarGridSpec(
            num_scalar_prefetch=2,
            grid=(blocks,),
            in_specs=[
                pl.BlockSpec((rows, width), mine),
                pl.BlockSpec(fresh.shape, whole),
                pl.BlockSpec(cache.shape, whole),
                pl.BlockSpec((1, rows), across),
                pl.BlockSpec((1, slot_count), whole),
                pl.BlockSpec((spans, HD), whole),
                pl.BlockSpec((spans, HD), whole),
            ],
            out_specs=pl.BlockSpec((rows, width), mine),
            scratch_shapes=[
                pltpu.VMEM((length, 2 * HD), jnp.bfloat16),
                pltpu.VMEM((HD + ONES, length), jnp.bfloat16),
                pltpu.VMEM((2 * HD, R), jnp.bfloat16),
                pltpu.VMEM((1, R), jnp.float32),
                pltpu.VMEM((HD + ONES, R), jnp.float32),
            ],
        ),
        out_shape=jax.ShapeDtypeStruct((slot_count, width), jnp.bfloat16),
        cost_estimate=pl.CostEstimate(
            flops=2 * elements * HD, bytes_accessed=16 * slot_count * width, transcendentals=elements // 2
        ),
        compiler_params=pltpu.CompilerParams(vmem_limit_bytes=60 * 2**20),
    )(bounds, edges, q, fresh, cache, chosen[None, :], chosen[None, :], acos, asin * signs)


def from_partner(value):
    pairs = [(source, source ^ 1) for source in range(lax.axis_size("col"))]
    return lax.ppermute(value, "col", pairs)


def shards(tokens, norm_gain, w_query, w_keyval, kv_cache, selected, anchor):
    chosen = selected[0]
    cosine, sine_part = angles(chosen.astype(jnp.float32), HD)
    queries, fresh = gather_and_project(
        tokens[0], norm_gain, w_query, w_keyval, cosine, signed(sine_part)
    )
    stored = kv_cache[0]
    if w_keyval.shape[1] == HD:
        holds_key = lax.axis_index("col") % 2 == 0

        def both(mine):
            partner = from_partner(mine)
            return jnp.concatenate(
                [jnp.where(holds_key, mine, partner), jnp.where(holds_key, partner, mine)], axis=1
            )

        stored, fresh = both(stored), both(fresh)
    return attend(queries, fresh, stored, chosen, anchor[0])[None]


def solution(mesh):
    in_specs = (
        P("row", None, "col"),
        P(),
        P("row", "col"),
        P("row", "col"),
        P("row", None, "col"),
        P("row", None),
        P("row", None),
    )
    out_specs = P("row", None, "col")
    return jax.shard_map(shards, mesh=mesh, in_specs=in_specs, out_specs=out_specs, check_vma=False)
```

```python
import functools
import math

import jax
import jax.numpy as jnp
from jax import lax
from jax.experimental import pallas as pl
from jax.experimental.pallas import tpu as pltpu
from jax.sharding import PartitionSpec as P

HD = 128
SPAN = 512
PAIR = 2
ONES = 16
TILE = 128

rope_base = 500000.0
epsilon = 1e-05
masked_score = -1e30
MESH = pl.DeviceIdType.MESH
VMEM = pl.BlockSpec(memory_space=pltpu.VMEM)
ANY = pl.BlockSpec(memory_space=pl.ANY)


def turn(vectors, cosine, signed_sine):
    return vectors * cosine + pltpu.roll(vectors, HD // 2, 1) * signed_sine


def project_kernel(
    cfg, tokens, gain, wq, wkv, chosen, q_out, kv_out, edges, firsts, lasts,
    x, weights_q, weights_kv, normed, cosine, sine, rx, to_right, to_left, to_pair, local, w_send, w_recv,
):
    ncol, nrow, chunks, total_length = cfg
    length = ncol // PAIR
    slots, width = tokens.shape
    rows = slots // chunks
    detour = chunks // 2
    per_row = wq.shape[0]
    q_width = wq.shape[1]
    kv_width = wkv.shape[1]
    col = lax.axis_index("col")
    row = lax.axis_index("row")
    place = lax.div(col, PAIR)
    side = lax.rem(col, PAIR)
    other = 1 - side
    has_right = place + 1 < length
    has_left = place > 0
    right = {"col": lax.rem(col + PAIR, ncol)}
    left = {"col": lax.rem(col + ncol - PAIR, ncol)}
    pair = {"col": col + 1 - 2 * side}
    row_bits = list(reversed(range(nrow.bit_length() - 1)))

    def flipped(index, bit):
        step = 2**bit
        return index + step - 2 * step * lax.rem(lax.div(index, step), 2)

    barrier = pltpu.get_barrier_semaphore()
    neighbours = [right, left, pair] + [{"row": flipped(row, bit)} for bit in row_bits]
    for device in neighbours:
        pl.semaphore_signal(barrier, inc=1, device_id=device, device_id_type=MESH)
    pl.semaphore_wait(barrier, len(neighbours))

    def span(i):
        return pl.ds(pl.multiple_of(i * rows, rows), rows)

    def block(at, which):
        return at * PAIR + which

    def moved(device, sems, sem, at, which, i, own=False):
        here = x.at[block(at, which), span(i), :]
        return pltpu.make_async_remote_copy(
            src_ref=tokens.at[span(i), :] if own else here,
            dst_ref=here,
            send_sem=sems.at[sem, i],
            recv_sem=rx.at[block(at, which), i],
            device_id=device,
            device_id_type=MESH,
        )

    def arrived(at, which, i):
        moved(pair, to_pair, 0, at, which, i).wait_recv()

    @pl.loop(0, chunks)
    def _(i):
        @pl.when(has_right)
        def _():
            moved(right, to_right, place, place, side, i, True).start()

        @pl.when(has_left)
        def _():
            moved(left, to_left, place, place, side, i, True).start()

        moved(pair, to_pair, place, place, side, i, True).start()

    def weight_copy(bit, mask, number):
        owner = row
        for b in row_bits:
            if mask & 2**b:
                owner = flipped(owner, b)
        at = pl.ds(pl.multiple_of(owner * per_row, per_row), per_row)
        pairs = [(wq, weights_q), (wkv, weights_kv)]
        return [
            pltpu.make_async_remote_copy(
                src_ref=source if mask == 0 else target.at[at],
                dst_ref=target.at[at],
                send_sem=w_send.at[number, j],
                recv_sem=w_recv.at[number, j],
                device_id={"row": flipped(row, bit)},
                device_id_type=MESH,
            )
            for j, (source, target) in enumerate(pairs)
        ]

    steps = []
    masks = [0]
    for bit in row_bits:
        steps += [(bit, mask) for mask in masks]
        masks += [mask ^ 2**bit for mask in masks]
    copies = [weight_copy(bit, mask, number) for number, (bit, mask) in enumerate(steps)]
    for (bit, mask), made in zip(steps, copies):
        if mask == 0:
            for copy in made:
                copy.start()
    mine = pl.ds(pl.multiple_of(row * per_row, per_row), per_row)
    own_copies = [
        pltpu.make_async_copy(tokens, x.at[col], local.at[0]),
        pltpu.make_async_copy(wq, weights_q.at[mine], local.at[1]),
        pltpu.make_async_copy(wkv, weights_kv.at[mine], local.at[2]),
    ]
    for copy in own_copies:
        copy.start()

    index = lax.broadcasted_iota(jnp.int32, (HD, TILE), 0)
    half = lax.rem(index, HD // 2).astype(jnp.float32)
    frequency = jnp.exp(half * (-2.0 / HD) * math.log(rope_base))
    sign = jnp.where(lax.broadcasted_iota(jnp.int32, (TILE, HD), 1) < HD // 2, -1.0, 1.0)
    marks = (lax.broadcasted_iota(jnp.int32, edges.shape, 0) * SPAN).astype(jnp.float32)
    below = jnp.zeros(edges.shape, jnp.float32)
    for t in range(slots // TILE):
        at = slice(t * TILE, (t + 1) * TILE)
        positions = chosen[:, at].astype(jnp.float32)
        phases = positions * frequency
        cosine[at, :] = jnp.cos(phases).T
        sine[at, :] = jnp.sin(phases).T * sign
        below = below + jnp.where(positions < marks, 1.0, 0.0)
        first = jnp.min(positions, axis=1, keepdims=True)
        last = jnp.max(jnp.where(positions < total_length, positions, 0.0), axis=1, keepdims=True)
        firsts[t : t + 1, :] = jnp.broadcast_to(first, (1, TILE)).astype(jnp.int32)
        lasts[t : t + 1, :] = jnp.broadcast_to(last, (1, TILE)).astype(jnp.int32)
    below = jnp.sum(below, axis=1, keepdims=True)
    edges[...] = jnp.broadcast_to(below, edges.shape).astype(jnp.int32)

    def hand_on(distance, i):
        def forward(at, onward_ok, onward, sems):
            arrived(at, side, i)

            @pl.when(onward_ok)
            def _():
                moved(onward, sems, at, at, side, i).start()

            if distance == 1:
                @pl.when(i < detour)
                def _():
                    moved(pair, to_pair, at, at, side, i).start()
            else:
                moved(pair, to_pair, at, at, side, i).start()

        @pl.when(place >= distance)
        def _():
            forward(place - distance, has_right, right, to_right)

        @pl.when(place + distance < length)
        def _():
            forward(place + distance, has_left, left, to_left)

        if distance == 1:
            arrived(place, other, i)

    def project(i):
        def squares(b, total):
            part = x[b, span(i), :].astype(jnp.float32)
            part = part * part
            for k in range(0, width, HD):
                total = total + part[:, k : k + HD]
            return total

        total = jnp.zeros((rows, HD), jnp.float32)
        for at in range(length):
            total = squares(block(at, side), total)
        for at in range(length):
            @pl.when(place != at)
            def _():
                arrived(at, other, i)
        for at in range(length):
            total = squares(block(at, other), total)
        mean_square = jnp.sum(total, axis=1, keepdims=True) / (ncol * width)
        scale = lax.rsqrt(mean_square + epsilon)
        cos, sin = cosine[span(i), :], sine[span(i), :]

        def heads(result, first):
            for k in range(0, result.shape[1], HD):
                part = turn(result[:, k : k + HD], cos, sin)
                q_out[span(i), first + k : first + k + HD] = part.astype(jnp.bfloat16)

        step = min(2 * HD, q_width)
        result = jnp.zeros((rows, step), jnp.float32)
        for b in range(ncol):
            at = slice(b * width, (b + 1) * width)
            part = x[b, span(i), :].astype(jnp.float32)
            part = (part * scale * gain[:, at].astype(jnp.float32)).astype(jnp.bfloat16)
            normed[:, at] = part
            result = result + jnp.dot(part, weights_q[at, :step], preferred_element_type=jnp.float32)
        heads(result, 0)
        for first in range(step, q_width, step):
            columns = weights_q[:, first : first + step]
            heads(jnp.dot(normed[...], columns, preferred_element_type=jnp.float32), first)
        result = jnp.dot(normed[...], weights_kv[...], preferred_element_type=jnp.float32)
        keys = result[:, :HD]
        turned = turn(keys, cos, sin)
        if kv_width == 2 * HD:
            kv_out[span(i), HD:] = result[:, HD:].astype(jnp.bfloat16)
        else:
            turned = jnp.where(lax.rem(col, 2) == 0, turned, keys)
        kv_out[span(i), :HD] = turned.astype(jnp.bfloat16)

    for distance in range(1, length - 1):
        @pl.loop(0, chunks)
        def _(i):
            hand_on(distance, i)

    @pl.loop(detour, chunks)
    def _(i):
        @pl.when(has_right)
        def _():
            moved(right, to_right, length - 1, place, other, i).start()

        @pl.when(has_left)
        def _():
            moved(left, to_left, 0, place, other, i).start()

    for number, (bit, mask) in enumerate(steps):
        if mask:
            came = [m for m, (b, k) in enumerate(steps) if k ^ 2**b == mask][0]
            for copy in copies[came]:
                copy.wait_recv()
            for copy in copies[number]:
                copy.start()
    forwarded = {mask for _, mask in steps}
    for number, (bit, mask) in enumerate(steps):
        if mask ^ 2**bit not in forwarded:
            for copy in copies[number]:
                copy.wait_recv()
    for copy in own_copies:
        copy.wait()

    ahead = min(chunks, 4)

    @pl.loop(0, chunks + ahead)
    def _(i):
        @pl.when(i < chunks)
        def _():
            hand_on(length - 1, i)

        @pl.when(i >= ahead)
        def _():
            project(i - ahead)

    @pl.loop(0, chunks)
    def _(i):
        late = i >= detour
        for at in range(length):
            @pl.when(has_right & (place >= at))
            def _():
                moved(right, to_right, at, at, side, i).wait_send()

            @pl.when(has_left & (place <= at))
            def _():
                moved(left, to_left, at, at, side, i).wait_send()

            near = (place - at == 1) | (at - place == 1)

            @pl.when(jnp.logical_not(near & late))
            def _():
                moved(pair, to_pair, at, at, side, i).wait_send()

        @pl.when(late & has_right)
        def _():
            moved(right, to_right, length - 1, place, other, i).wait_send()

        @pl.when(late & has_left)
        def _():
            moved(left, to_left, 0, place, other, i).wait_send()

    for made in copies:
        for copy in made:
            copy.wait_send()


def gather_and_project(tokens, norm_gain, w_query, w_keyval, selected, total_length):
    ncol, nrow = lax.axis_size("col"), lax.axis_size("row")
    slots, width = tokens.shape
    depth, q_width = w_query.shape
    kv_width = w_keyval.shape[1]
    chunks = next(n for n in (6, 4, 3, 2, 1) if slots % (n * 16) == 0)
    rows = slots // chunks
    features = ncol * width
    length = ncol // PAIR
    moves = nrow - 1
    dma = pltpu.SemaphoreType.DMA
    outs = (
        jax.ShapeDtypeStruct((slots, q_width), jnp.bfloat16),
        jax.ShapeDtypeStruct((slots, kv_width), jnp.bfloat16),
        jax.ShapeDtypeStruct((-(-(total_length // SPAN + 1) // 8) * 8, TILE), jnp.int32),
        jax.ShapeDtypeStruct((slots // TILE, TILE), jnp.int32),
        jax.ShapeDtypeStruct((slots // TILE, TILE), jnp.int32),
    )
    return pl.pallas_call(
        functools.partial(project_kernel, (ncol, nrow, chunks, total_length)),
        out_shape=outs,
        in_specs=[ANY, VMEM, ANY, ANY, VMEM],
        out_specs=(VMEM,) * 5,
        scratch_shapes=[
            pltpu.VMEM((ncol, slots, width), jnp.bfloat16),
            pltpu.VMEM((features, q_width), jnp.bfloat16),
            pltpu.VMEM((features, kv_width), jnp.bfloat16),
            pltpu.VMEM((rows, features), jnp.bfloat16),
            pltpu.VMEM((slots, HD), jnp.float32),
            pltpu.VMEM((slots, HD), jnp.float32),
            dma((ncol, chunks)),
            dma((length, chunks)),
            dma((length, chunks)),
            dma((length, chunks)),
            dma((3,)),
            dma((moves, 2)),
            dma((moves, 2)),
        ],
        compiler_params=pltpu.CompilerParams(
            collective_id=0, has_side_effects=True, vmem_limit_bytes=62 * 2**20
        ),
        cost_estimate=pl.CostEstimate(
            flops=2 * slots * features * (q_width + kv_width),
            bytes_accessed=2 * (slots * features + features * (q_width + kv_width)),
            transcendentals=0,
        ),
    )(
        tokens,
        norm_gain[None, :],
        w_query,
        w_keyval,
        selected,
    )


def attend_kernel(
    cfg, edges, firsts, lasts, anchor, q, fresh, cache, chosen, chosen_row, out, keys, values, qt, m, acc, acos, asin
):
    heads, length, wide, narrow, group = cfg
    block = pl.program_id(0)
    rows = q.shape[0]
    factor = HD ** (-0.5) * math.log2(math.e)
    spans = length // SPAN

    @pl.when(block == 0)
    def _():
        ones = jnp.ones((TILE, HD), jnp.bfloat16)
        for c in range(spans):
            acos[c : c + 1, :] = jnp.full((1, HD), (c * SPAN - anchor[0, c]).astype(jnp.float32))
        lane = lax.broadcasted_iota(jnp.int32, acos.shape, 1)
        half = lax.rem(lane, HD // 2).astype(jnp.float32)
        phases = acos[...] * jnp.exp(half * (-2.0 / HD) * math.log(rope_base))
        asin[...] = jnp.sin(phases) * jnp.where(lane < HD // 2, -1.0, 1.0)
        acos[...] = jnp.cos(phases)

        def prepare(c, carry):
            base = pl.multiple_of(c * SPAN, SPAN)
            stored = cache[pl.ds(base, SPAN), :]
            old = stored[:, :HD].astype(jnp.float32)
            turned = old * acos[pl.ds(c, 1), :] + pltpu.roll(old, HD // 2, 1) * asin[pl.ds(c, 1), :]
            keys[pl.ds(base, SPAN), :HD] = turned.astype(jnp.bfloat16)
            keys[pl.ds(base, SPAN), HD:] = stored[:, HD:]

            def blend(tile, carry):
                at = pl.multiple_of(tile * TILE, TILE)
                place = base + lax.broadcasted_iota(jnp.int32, (SPAN, TILE), 0)
                hits = (place == chosen_row[:, pl.ds(at, TILE)]).astype(jnp.float32).astype(jnp.bfloat16)
                fresh_tile = jnp.concatenate([fresh[pl.ds(at, TILE), :], ones], axis=1)
                placed = jnp.dot(hits, fresh_tile, preferred_element_type=jnp.float32)
                hit = placed[:, 2 * HD :] > 0.5
                for k in (0, HD):
                    before = keys[pl.ds(base, SPAN), k : k + HD].astype(jnp.float32)
                    after = jnp.where(hit, placed[:, k : k + HD], before)
                    keys[pl.ds(base, SPAN), k : k + HD] = after.astype(jnp.bfloat16)
                return carry

            lax.fori_loop(edges[c, 0] // TILE, (edges[c + 1, 0] + TILE - 1) // TILE, blend, 0)
            values[:HD, pl.ds(base, SPAN)] = keys[pl.ds(base, SPAN), HD:].astype(jnp.float32).T.astype(jnp.bfloat16)
            values[HD:, pl.ds(base, SPAN)] = jnp.ones((ONES, SPAN), jnp.bfloat16)
            keys[pl.ds(base, SPAN), HD:] = keys[pl.ds(base, SPAN), :HD]
            return carry

        lax.fori_loop(0, spans, prepare, 0)

    for h in range(heads):
        scaled = (q[:, h * HD : (h + 1) * HD].astype(jnp.float32) * factor).T
        high = scaled.astype(jnp.bfloat16)
        qt[:HD, h * rows : (h + 1) * rows] = high
        qt[HD:, h * rows : (h + 1) * rows] = (scaled - high.astype(jnp.float32)).astype(jnp.bfloat16)
    m[...] = jnp.full(m.shape, masked_score, jnp.float32)
    acc[...] = jnp.zeros(acc.shape, jnp.float32)
    limit = chosen[...]
    limits = jnp.concatenate([limit] * (group // rows), axis=1) if group > rows else limit

    def advance(size, masked, index, carry):
        start = pl.multiple_of(index * size, size)
        key_block = keys[pl.ds(start, size), :]
        value_block = values[:, pl.ds(start, size)]
        for at in range(0, heads * rows, group):
            scores = jnp.dot(key_block, qt[:, at : at + group], preferred_element_type=jnp.float32)
            if masked:
                place = start + lax.broadcasted_iota(jnp.int32, scores.shape, 0)
                scores = jnp.where(place <= limits, scores, masked_score)
            old = m[:, at : at + group]
            new = jnp.maximum(old, jnp.max(scores, axis=0, keepdims=True))
            weights = jnp.exp2(scores - new).astype(jnp.bfloat16)
            part = jnp.dot(value_block, weights, preferred_element_type=jnp.float32)
            acc[:, at : at + group] = acc[:, at : at + group] * jnp.exp2(old - new) + part
            m[:, at : at + group] = new
        return carry

    farthest = lasts[block, 0]
    total = farthest // narrow + 1
    full = jnp.minimum((firsts[block, 0] + 1) // wide, (farthest + 1) // wide)
    lax.fori_loop(0, full, functools.partial(advance, wide, False), 0)
    lax.fori_loop(full * (wide // narrow), total, functools.partial(advance, narrow, True), 0)
    for h in range(heads):
        part = acc[:, h * rows : (h + 1) * rows]
        outcome = jnp.where(limit < length, part[:HD, :] / part[HD : HD + 1, :], 0.0)
        out[:, h * HD : (h + 1) * HD] = outcome.T.astype(out.dtype)


def attend(q, fresh, cache, selected, anchor, edges, firsts, lasts):
    slot_count, width = q.shape
    length = cache.shape[0]
    heads = width // HD
    rows = TILE
    blocks = slot_count // rows
    spans = length // SPAN
    narrow = SPAN
    wide = next(n for n in (4 * SPAN, 2 * SPAN, SPAN) if length % n == 0)
    group = heads * rows
    mine = lambda i, *_: (i, 0)
    across = lambda i, *_: (0, i)
    whole = lambda i, *_: (0, 0)
    R = heads * rows
    elements = slot_count * heads * length
    return pl.pallas_call(
        functools.partial(attend_kernel, (heads, length, wide, narrow, group)),
        grid_spec=pltpu.PrefetchScalarGridSpec(
            num_scalar_prefetch=4,
            grid=(blocks,),
            in_specs=[
                pl.BlockSpec((rows, width), mine),
                pl.BlockSpec(fresh.shape, whole),
                pl.BlockSpec(cache.shape, whole),
                pl.BlockSpec((1, rows), across),
                pl.BlockSpec((1, slot_count), whole),
            ],
            out_specs=pl.BlockSpec((rows, width), mine),
            scratch_shapes=[
                pltpu.VMEM((length, 2 * HD), jnp.bfloat16),
                pltpu.VMEM((HD + ONES, length), jnp.bfloat16),
                pltpu.VMEM((2 * HD, R), jnp.bfloat16),
                pltpu.VMEM((1, R), jnp.float32),
                pltpu.VMEM((HD + ONES, R), jnp.float32),
                pltpu.VMEM((spans, HD), jnp.float32),
                pltpu.VMEM((spans, HD), jnp.float32),
            ],
        ),
        out_shape=jax.ShapeDtypeStruct((slot_count, width), jnp.bfloat16),
        cost_estimate=pl.CostEstimate(
            flops=2 * elements * HD, bytes_accessed=16 * slot_count * width, transcendentals=elements // 2
        ),
        compiler_params=pltpu.CompilerParams(vmem_limit_bytes=60 * 2**20),
    )(edges, firsts, lasts, anchor, q, fresh, cache, selected, selected)


def from_partner(value):
    pairs = [(source, source ^ 1) for source in range(lax.axis_size("col"))]
    return lax.ppermute(value, "col", pairs)


def shards(tokens, norm_gain, w_query, w_keyval, kv_cache, selected, anchor):
    stored = kv_cache[0]
    queries, fresh, *tables = gather_and_project(
        tokens[0], norm_gain, w_query, w_keyval, selected, stored.shape[0]
    )
    if w_keyval.shape[1] == HD:
        holds_key = lax.axis_index("col") % 2 == 0

        def both(mine):
            partner = from_partner(mine)
            return jnp.concatenate(
                [jnp.where(holds_key, mine, partner), jnp.where(holds_key, partner, mine)], axis=1
            )

        stored, fresh = both(stored), both(fresh)
    return attend(queries, fresh, stored, selected, anchor, *tables)[None]


def solution(mesh):
    in_specs = (
        P("row", None, "col"),
        P(),
        P("row", "col"),
        P("row", "col"),
        P("row", None, "col"),
        P("row", None),
        P("row", None),
    )
    out_specs = P("row", None, "col")
    return jax.shard_map(shards, mesh=mesh, in_specs=in_specs, out_specs=out_specs, check_vma=False)
```

```python
import functools
import math

import jax
import jax.numpy as jnp
from jax import lax
from jax.experimental import pallas as pl
from jax.experimental.pallas import tpu as pltpu
from jax.sharding import PartitionSpec as P

HD = 128
SPAN = 512
PAIR = 2
ONES = 16
TILE = 128

rope_base = 500000.0
epsilon = 1e-05
masked_score = -1e30
MESH = pl.DeviceIdType.MESH
VMEM = pl.BlockSpec(memory_space=pltpu.VMEM)
ANY = pl.BlockSpec(memory_space=pl.ANY)


def turn(vectors, cosine, signed_sine):
    return vectors * cosine + pltpu.roll(vectors, HD // 2, 1) * signed_sine


def project_kernel(
    cfg, tokens, gain, wq, wkv, chosen, q_out, kv_out, edges, firsts, lasts,
    x, weights_q, weights_kv, normed, cosine, sine, rx, to_right, to_left, to_pair, local, w_send, w_recv,
):
    ncol, nrow, chunks, total_length = cfg
    length = ncol // PAIR
    slots, width = tokens.shape
    rows = slots // chunks
    detour = chunks // 2
    per_row = wq.shape[0]
    q_width = wq.shape[1]
    kv_width = wkv.shape[1]
    col = lax.axis_index("col")
    row = lax.axis_index("row")
    place = lax.div(col, PAIR)
    side = lax.rem(col, PAIR)
    other = 1 - side
    has_right = place + 1 < length
    has_left = place > 0
    right = {"col": lax.rem(col + PAIR, ncol)}
    left = {"col": lax.rem(col + ncol - PAIR, ncol)}
    pair = {"col": col + 1 - 2 * side}
    row_bits = list(reversed(range(nrow.bit_length() - 1)))

    def flipped(index, bit):
        step = 2**bit
        return index + step - 2 * step * lax.rem(lax.div(index, step), 2)

    barrier = pltpu.get_barrier_semaphore()
    neighbours = [right, left, pair] + [{"row": flipped(row, bit)} for bit in row_bits]
    for device in neighbours:
        pl.semaphore_signal(barrier, inc=1, device_id=device, device_id_type=MESH)
    pl.semaphore_wait(barrier, len(neighbours))

    def span(i):
        return pl.ds(pl.multiple_of(i * rows, rows), rows)

    def block(at, which):
        return at * PAIR + which

    def moved(device, sems, sem, at, which, i, own=False):
        here = x.at[block(at, which), span(i), :]
        return pltpu.make_async_remote_copy(
            src_ref=tokens.at[span(i), :] if own else here,
            dst_ref=here,
            send_sem=sems.at[sem, i],
            recv_sem=rx.at[block(at, which), i],
            device_id=device,
            device_id_type=MESH,
        )

    def arrived(at, which, i):
        moved(pair, to_pair, 0, at, which, i).wait_recv()

    @pl.loop(0, chunks)
    def _(i):
        @pl.when(has_right)
        def _():
            moved(right, to_right, place, place, side, i, True).start()

        @pl.when(has_left)
        def _():
            moved(left, to_left, place, place, side, i, True).start()

        moved(pair, to_pair, place, place, side, i, True).start()

    def weight_copy(bit, mask, number):
        owner = row
        for b in row_bits:
            if mask & 2**b:
                owner = flipped(owner, b)
        at = pl.ds(pl.multiple_of(owner * per_row, per_row), per_row)
        pairs = [(wq, weights_q), (wkv, weights_kv)]
        return [
            pltpu.make_async_remote_copy(
                src_ref=source if mask == 0 else target.at[at],
                dst_ref=target.at[at],
                send_sem=w_send.at[number, j],
                recv_sem=w_recv.at[number, j],
                device_id={"row": flipped(row, bit)},
                device_id_type=MESH,
            )
            for j, (source, target) in enumerate(pairs)
        ]

    steps = []
    masks = [0]
    for bit in row_bits:
        steps += [(bit, mask) for mask in masks]
        masks += [mask ^ 2**bit for mask in masks]
    copies = [weight_copy(bit, mask, number) for number, (bit, mask) in enumerate(steps)]
    for (bit, mask), made in zip(steps, copies):
        if mask == 0:
            for copy in made:
                copy.start()
    mine = pl.ds(pl.multiple_of(row * per_row, per_row), per_row)
    own_copies = [
        pltpu.make_async_copy(tokens, x.at[col], local.at[0]),
        pltpu.make_async_copy(wq, weights_q.at[mine], local.at[1]),
        pltpu.make_async_copy(wkv, weights_kv.at[mine], local.at[2]),
    ]
    for copy in own_copies:
        copy.start()

    index = lax.broadcasted_iota(jnp.int32, (HD, TILE), 0)
    half = lax.rem(index, HD // 2).astype(jnp.float32)
    frequency = jnp.exp(half * (-2.0 / HD) * math.log(rope_base))
    sign = jnp.where(lax.broadcasted_iota(jnp.int32, (TILE, HD), 1) < HD // 2, -1.0, 1.0)
    marks = (lax.broadcasted_iota(jnp.int32, edges.shape, 0) * SPAN).astype(jnp.float32)
    below = jnp.zeros(edges.shape, jnp.float32)
    for t in range(slots // TILE):
        at = slice(t * TILE, (t + 1) * TILE)
        positions = chosen[:, at].astype(jnp.float32)
        phases = positions * frequency
        cosine[at, :] = jnp.cos(phases).T
        sine[at, :] = jnp.sin(phases).T * sign
        below = below + jnp.where(positions < marks, 1.0, 0.0)
        first = jnp.min(positions, axis=1, keepdims=True)
        last = jnp.max(jnp.where(positions < total_length, positions, 0.0), axis=1, keepdims=True)
        firsts[t : t + 1, :] = jnp.broadcast_to(first, (1, TILE)).astype(jnp.int32)
        lasts[t : t + 1, :] = jnp.broadcast_to(last, (1, TILE)).astype(jnp.int32)
    below = jnp.sum(below, axis=1, keepdims=True)
    edges[...] = jnp.broadcast_to(below, edges.shape).astype(jnp.int32)

    def hand_on(distance, i):
        def forward(at, onward_ok, onward, sems):
            arrived(at, side, i)

            @pl.when(onward_ok)
            def _():
                moved(onward, sems, at, at, side, i).start()

            if distance == 1:
                @pl.when(i < detour)
                def _():
                    moved(pair, to_pair, at, at, side, i).start()
            else:
                moved(pair, to_pair, at, at, side, i).start()

        @pl.when(place >= distance)
        def _():
            forward(place - distance, has_right, right, to_right)

        @pl.when(place + distance < length)
        def _():
            forward(place + distance, has_left, left, to_left)

        if distance == 1:
            arrived(place, other, i)

    def project(i):
        def squares(b, total):
            part = x[b, span(i), :].astype(jnp.float32)
            part = part * part
            for k in range(0, width, HD):
                total = total + part[:, k : k + HD]
            return total

        total = jnp.zeros((rows, HD), jnp.float32)
        for at in range(length):
            total = squares(block(at, side), total)
        for at in range(length):
            @pl.when(place != at)
            def _():
                arrived(at, other, i)
        for at in range(length):
            total = squares(block(at, other), total)
        mean_square = jnp.sum(total, axis=1, keepdims=True) / (ncol * width)
        scale = lax.rsqrt(mean_square + epsilon)
        cos, sin = cosine[span(i), :], sine[span(i), :]

        def heads(result, first):
            for k in range(0, result.shape[1], HD):
                part = turn(result[:, k : k + HD], cos, sin)
                q_out[span(i), first + k : first + k + HD] = part.astype(jnp.bfloat16)

        step = min(2 * HD, q_width)
        result = jnp.zeros((rows, step), jnp.float32)
        for b in range(ncol):
            at = slice(b * width, (b + 1) * width)
            part = x[b, span(i), :].astype(jnp.float32)
            part = (part * scale * gain[:, at].astype(jnp.float32)).astype(jnp.bfloat16)
            normed[:, at] = part
            result = result + jnp.dot(part, weights_q[at, :step], preferred_element_type=jnp.float32)
        heads(result, 0)
        for first in range(step, q_width, step):
            columns = weights_q[:, first : first + step]
            heads(jnp.dot(normed[...], columns, preferred_element_type=jnp.float32), first)
        result = jnp.dot(normed[...], weights_kv[...], preferred_element_type=jnp.float32)
        keys = result[:, :HD]
        turned = turn(keys, cos, sin)
        if kv_width == 2 * HD:
            kv_out[span(i), HD:] = result[:, HD:].astype(jnp.bfloat16)
        else:
            turned = jnp.where(lax.rem(col, 2) == 0, turned, keys)
        kv_out[span(i), :HD] = turned.astype(jnp.bfloat16)

    for distance in range(1, length - 1):
        @pl.loop(0, chunks)
        def _(i):
            hand_on(distance, i)

    @pl.loop(detour, chunks)
    def _(i):
        @pl.when(has_right)
        def _():
            moved(right, to_right, length - 1, place, other, i).start()

        @pl.when(has_left)
        def _():
            moved(left, to_left, 0, place, other, i).start()

    for number, (bit, mask) in enumerate(steps):
        if mask:
            came = [m for m, (b, k) in enumerate(steps) if k ^ 2**b == mask][0]
            for copy in copies[came]:
                copy.wait_recv()
            for copy in copies[number]:
                copy.start()
    forwarded = {mask for _, mask in steps}
    for number, (bit, mask) in enumerate(steps):
        if mask ^ 2**bit not in forwarded:
            for copy in copies[number]:
                copy.wait_recv()
    for copy in own_copies:
        copy.wait()

    ahead = min(chunks, 4)

    @pl.loop(0, chunks + ahead)
    def _(i):
        @pl.when(i < chunks)
        def _():
            hand_on(length - 1, i)

        @pl.when(i >= ahead)
        def _():
            project(i - ahead)

    @pl.loop(0, chunks)
    def _(i):
        late = i >= detour
        for at in range(length):
            @pl.when(has_right & (place >= at))
            def _():
                moved(right, to_right, at, at, side, i).wait_send()

            @pl.when(has_left & (place <= at))
            def _():
                moved(left, to_left, at, at, side, i).wait_send()

            near = (place - at == 1) | (at - place == 1)

            @pl.when(jnp.logical_not(near & late))
            def _():
                moved(pair, to_pair, at, at, side, i).wait_send()

        @pl.when(late & has_right)
        def _():
            moved(right, to_right, length - 1, place, other, i).wait_send()

        @pl.when(late & has_left)
        def _():
            moved(left, to_left, 0, place, other, i).wait_send()

    for made in copies:
        for copy in made:
            copy.wait_send()


def gather_and_project(tokens, norm_gain, w_query, w_keyval, selected, total_length):
    ncol, nrow = lax.axis_size("col"), lax.axis_size("row")
    slots, width = tokens.shape
    depth, q_width = w_query.shape
    kv_width = w_keyval.shape[1]
    chunks = next(n for n in (6, 4, 3, 2, 1) if slots % (n * 16) == 0)
    rows = slots // chunks
    features = ncol * width
    length = ncol // PAIR
    moves = nrow - 1
    dma = pltpu.SemaphoreType.DMA
    outs = (
        jax.ShapeDtypeStruct((slots, q_width), jnp.bfloat16),
        jax.ShapeDtypeStruct((slots, kv_width), jnp.bfloat16),
        jax.ShapeDtypeStruct((-(-(total_length // SPAN + 1) // 8) * 8, TILE), jnp.int32),
        jax.ShapeDtypeStruct((slots // TILE, TILE), jnp.int32),
        jax.ShapeDtypeStruct((slots // TILE, TILE), jnp.int32),
    )
    return pl.pallas_call(
        functools.partial(project_kernel, (ncol, nrow, chunks, total_length)),
        out_shape=outs,
        in_specs=[ANY, VMEM, ANY, ANY, VMEM],
        out_specs=(VMEM,) * 5,
        scratch_shapes=[
            pltpu.VMEM((ncol, slots, width), jnp.bfloat16),
            pltpu.VMEM((features, q_width), jnp.bfloat16),
            pltpu.VMEM((features, kv_width), jnp.bfloat16),
            pltpu.VMEM((rows, features), jnp.bfloat16),
            pltpu.VMEM((slots, HD), jnp.float32),
            pltpu.VMEM((slots, HD), jnp.float32),
            dma((ncol, chunks)),
            dma((length, chunks)),
            dma((length, chunks)),
            dma((length, chunks)),
            dma((3,)),
            dma((moves, 2)),
            dma((moves, 2)),
        ],
        compiler_params=pltpu.CompilerParams(
            collective_id=0, has_side_effects=True, vmem_limit_bytes=62 * 2**20
        ),
        cost_estimate=pl.CostEstimate(
            flops=2 * slots * features * (q_width + kv_width),
            bytes_accessed=2 * (slots * features + features * (q_width + kv_width)),
            transcendentals=0,
        ),
    )(
        tokens,
        norm_gain[None, :],
        w_query,
        w_keyval,
        selected,
    )


def attend_kernel(
    cfg, edges, firsts, lasts, anchor, q, fresh, cache, chosen, chosen_row, out, keys, values, qt, m, acc, acos, asin
):
    heads, length, sizes, narrow, group = cfg
    block = pl.program_id(0)
    rows = q.shape[0]
    factor = HD ** (-0.5) * math.log2(math.e)
    spans = length // SPAN

    @pl.when(block == 0)
    def _():
        ones = jnp.ones((TILE, HD), jnp.bfloat16)
        for c in range(spans):
            acos[c : c + 1, :] = jnp.full((1, HD), (c * SPAN - anchor[0, c]).astype(jnp.float32))
        lane = lax.broadcasted_iota(jnp.int32, acos.shape, 1)
        half = lax.rem(lane, HD // 2).astype(jnp.float32)
        phases = acos[...] * jnp.exp(half * (-2.0 / HD) * math.log(rope_base))
        asin[...] = jnp.sin(phases) * jnp.where(lane < HD // 2, -1.0, 1.0)
        acos[...] = jnp.cos(phases)

        def prepare(c, carry):
            base = pl.multiple_of(c * SPAN, SPAN)
            stored = cache[pl.ds(base, SPAN), :]
            old = stored[:, :HD].astype(jnp.float32)
            turned = old * acos[pl.ds(c, 1), :] + pltpu.roll(old, HD // 2, 1) * asin[pl.ds(c, 1), :]
            keys[pl.ds(base, SPAN), :HD] = turned.astype(jnp.bfloat16)
            keys[pl.ds(base, SPAN), HD:] = stored[:, HD:]

            def blend(tile, carry):
                at = pl.multiple_of(tile * TILE, TILE)
                place = base + lax.broadcasted_iota(jnp.int32, (SPAN, TILE), 0)
                hits = (place == chosen_row[:, pl.ds(at, TILE)]).astype(jnp.float32).astype(jnp.bfloat16)
                fresh_tile = jnp.concatenate([fresh[pl.ds(at, TILE), :], ones], axis=1)
                placed = jnp.dot(hits, fresh_tile, preferred_element_type=jnp.float32)
                hit = placed[:, 2 * HD :] > 0.5
                for k in (0, HD):
                    before = keys[pl.ds(base, SPAN), k : k + HD].astype(jnp.float32)
                    after = jnp.where(hit, placed[:, k : k + HD], before)
                    keys[pl.ds(base, SPAN), k : k + HD] = after.astype(jnp.bfloat16)
                return carry

            lax.fori_loop(edges[c, 0] // TILE, (edges[c + 1, 0] + TILE - 1) // TILE, blend, 0)
            values[:HD, pl.ds(base, SPAN)] = keys[pl.ds(base, SPAN), HD:].astype(jnp.float32).T.astype(jnp.bfloat16)
            values[HD:, pl.ds(base, SPAN)] = jnp.ones((ONES, SPAN), jnp.bfloat16)
            keys[pl.ds(base, SPAN), HD:] = keys[pl.ds(base, SPAN), :HD]
            return carry

        lax.fori_loop(0, spans, prepare, 0)

    for h in range(heads):
        scaled = (q[:, h * HD : (h + 1) * HD].astype(jnp.float32) * factor).T
        high = scaled.astype(jnp.bfloat16)
        qt[:HD, h * rows : (h + 1) * rows] = high
        qt[HD:, h * rows : (h + 1) * rows] = (scaled - high.astype(jnp.float32)).astype(jnp.bfloat16)
    m[...] = jnp.full(m.shape, masked_score, jnp.float32)
    acc[...] = jnp.zeros(acc.shape, jnp.float32)
    limit = chosen[...]
    limits = jnp.concatenate([limit] * (group // rows), axis=1) if group > rows else limit

    def advance(size, masked, index, carry):
        start = pl.multiple_of(index * size, size)
        key_block = keys[pl.ds(start, size), :]
        value_block = values[:, pl.ds(start, size)]
        for at in range(0, heads * rows, group):
            scores = jnp.dot(key_block, qt[:, at : at + group], preferred_element_type=jnp.float32)
            if masked:
                place = start + lax.broadcasted_iota(jnp.int32, scores.shape, 0)
                scores = jnp.where(place <= limits, scores, masked_score)
            old = m[:, at : at + group]
            new = jnp.maximum(old, jnp.max(scores, axis=0, keepdims=True))
            weights = jnp.exp2(scores - new).astype(jnp.bfloat16)
            part = jnp.dot(value_block, weights, preferred_element_type=jnp.float32)
            acc[:, at : at + group] = acc[:, at : at + group] * jnp.exp2(old - new) + part
            m[:, at : at + group] = new
        return carry

    farthest = lasts[block, 0]
    total = farthest // narrow + 1
    free = jnp.minimum(firsts[block, 0] + 1, farthest + 1) // narrow
    done = 0
    for size in sizes:
        units = size // narrow
        lax.fori_loop(done // units, free // units, functools.partial(advance, size, False), 0)
        done = free // units * units
    lax.fori_loop(done, total, functools.partial(advance, narrow, True), 0)
    for h in range(heads):
        part = acc[:, h * rows : (h + 1) * rows]
        outcome = jnp.where(limit < length, part[:HD, :] / part[HD : HD + 1, :], 0.0)
        out[:, h * HD : (h + 1) * HD] = outcome.T.astype(out.dtype)


def attend(q, fresh, cache, selected, anchor, edges, firsts, lasts):
    slot_count, width = q.shape
    length = cache.shape[0]
    heads = width // HD
    rows = TILE
    blocks = slot_count // rows
    spans = length // SPAN
    narrow = SPAN
    sizes = [n * SPAN for n in (8, 4, 2) if length % (n * SPAN) == 0]
    group = heads * rows
    mine = lambda i, *_: (i, 0)
    across = lambda i, *_: (0, i)
    whole = lambda i, *_: (0, 0)
    R = heads * rows
    elements = slot_count * heads * length
    return pl.pallas_call(
        functools.partial(attend_kernel, (heads, length, sizes, narrow, group)),
        grid_spec=pltpu.PrefetchScalarGridSpec(
            num_scalar_prefetch=4,
            grid=(blocks,),
            in_specs=[
                pl.BlockSpec((rows, width), mine),
                pl.BlockSpec(fresh.shape, whole),
                pl.BlockSpec(cache.shape, whole),
                pl.BlockSpec((1, rows), across),
                pl.BlockSpec((1, slot_count), whole),
            ],
            out_specs=pl.BlockSpec((rows, width), mine),
            scratch_shapes=[
                pltpu.VMEM((length, 2 * HD), jnp.bfloat16),
                pltpu.VMEM((HD + ONES, length), jnp.bfloat16),
                pltpu.VMEM((2 * HD, R), jnp.bfloat16),
                pltpu.VMEM((1, R), jnp.float32),
                pltpu.VMEM((HD + ONES, R), jnp.float32),
                pltpu.VMEM((spans, HD), jnp.float32),
                pltpu.VMEM((spans, HD), jnp.float32),
            ],
        ),
        out_shape=jax.ShapeDtypeStruct((slot_count, width), jnp.bfloat16),
        cost_estimate=pl.CostEstimate(
            flops=2 * elements * HD, bytes_accessed=16 * slot_count * width, transcendentals=elements // 2
        ),
        compiler_params=pltpu.CompilerParams(vmem_limit_bytes=60 * 2**20),
    )(edges, firsts, lasts, anchor, q, fresh, cache, selected, selected)


def from_partner(value):
    pairs = [(source, source ^ 1) for source in range(lax.axis_size("col"))]
    return lax.ppermute(value, "col", pairs)


def shards(tokens, norm_gain, w_query, w_keyval, kv_cache, selected, anchor):
    stored = kv_cache[0]
    queries, fresh, *tables = gather_and_project(
        tokens[0], norm_gain, w_query, w_keyval, selected, stored.shape[0]
    )
    if w_keyval.shape[1] == HD:
        holds_key = lax.axis_index("col") % 2 == 0

        def both(mine):
            partner = from_partner(mine)
            return jnp.concatenate(
                [jnp.where(holds_key, mine, partner), jnp.where(holds_key, partner, mine)], axis=1
            )

        stored, fresh = both(stored), both(fresh)
    return attend(queries, fresh, stored, selected, anchor, *tables)[None]


def solution(mesh):
    in_specs = (
        P("row", None, "col"),
        P(),
        P("row", "col"),
        P("row", "col"),
        P("row", None, "col"),
        P("row", None),
        P("row", None),
    )
    out_specs = P("row", None, "col")
    return jax.shard_map(shards, mesh=mesh, in_specs=in_specs, out_specs=out_specs, check_vma=False)
```
